32 devices in a mesh: tile: 8 (over z, x), dir: 4 (over y, core).
Axes of the slice: x: 2, y: 2, z: 4, core: 2. Of those that a mesh axis runs over, the one named last changes fastest.
Arguments:
- layers: bfloat16 [4, 1024, 2048], P('dir', 'tile'), may hold values from -6 to 6
- offsets: int32 [4, 4, 2], replicated, may hold values from 0 to 8191, as said below
- subap_valid: int32 [8, 16], P('tile'), may hold values from 0 to 1, as said below
- defocus: float32 [3], replicated, may hold values from -0.08 to 0.08
- weights: float32 [3], replicated, may hold values from 0.25 to 1
Outputs:
- spots: bfloat16 [4, 8, 128, 2048], P('dir', 'tile')
The draws below stay inside these ranges and needn't reach their ends.
Inputs may be any that keep to these rules, and one draw needn't show every extreme that they name: offsets[d, l, 0] < 1024 and offsets[d, l, 1] < 8192; both bounds minus one are taken by some pair in every draw. `subap_valid`: the part of an annulus of lit subapertures that falls in the strip, with a few dead ones.
All inputs are finite; a program needn't handle non-finite values.
Results may differ from the reference program's by a relative error of at most 0.0055.
Values may be sent and summed in bfloat16 or wider, within the bound.
A program may use at most 64 MiB of HBM per device.

```python
import math
import jax
import jax.numpy as jnp
from jax import lax

SUBPIX = 128
SPOT = 128
SUBX = 16
SLICES = 3
REACH = 2
QUANT = 4
OVER = 2
ROWS = 8
PCOLS = 2048
DIRS = 4
LAYERS = 4


def draw_offsets(key, part):
    keys = jax.random.split(jax.random.fold_in(key, 11), 3)
    row_bound = REACH * SUBPIX * QUANT
    col_bound = PCOLS * QUANT
    row_values = jax.random.randint(keys[0], (DIRS * LAYERS,), 0, row_bound, dtype=jnp.int32)
    col_values = jax.random.randint(keys[1], (DIRS * LAYERS,), 0, col_bound, dtype=jnp.int32)
    chosen = jax.random.permutation(keys[2], DIRS * LAYERS)
    row_values = row_values.at[chosen[0]].set(row_bound - 1).at[chosen[1]].set(0)
    col_values = col_values.at[chosen[2]].set(col_bound - 1)
    return jnp.stack([row_values, col_values], 1).reshape(DIRS, LAYERS, 2).astype(jnp.int32)


def draw_subap_valid(key, part):
    keys = jax.random.split(jax.random.fold_in(key, 23), 5)
    centre_row = jax.random.randint(keys[0], (), -4, 5, dtype=jnp.int32)
    outer_share = jax.random.randint(keys[2], (), 30, 71, dtype=jnp.int32)
    inner_most = (2 * SUBX - 1) * (2 * SUBX - 1) // 2 + 1
    inner = jax.random.randint(keys[3], (), 1, inner_most + 1, dtype=jnp.int32)
    row_twice = 2 * jnp.arange(ROWS, dtype=jnp.int32)[:, None] - (ROWS - 1) - centre_row
    col_twice = 2 * jnp.arange(SUBX, dtype=jnp.int32)[None, :] + 1
    radius = row_twice * row_twice + col_twice * col_twice
    outer = (ROWS + 4) * (ROWS + 4) + 4 * SUBX * SUBX * outer_share // 100
    alive = jax.random.randint(keys[4], (ROWS, SUBX), 0, 32, dtype=jnp.int32) != 0
    lit = (radius <= outer) & (radius >= inner) & alive
    return jnp.where(lit, 1, 0).astype(jnp.int32)


def level_of(own_key, dims, pieces, least, largest):
    def one(dim, blocks):
        heights = jax.random.uniform(jax.random.fold_in(jax.random.fold_in(own_key, 6), dim), (blocks,), jnp.float32, least / len(pieces), largest / len(pieces))
        return jnp.repeat(jnp.exp(heights), dims[dim] // blocks).reshape((-1,) + (1,) * (len(dims) - dim - 1))

    level = one(*pieces[0])
    for cut in pieces[1:]:
        level = level * one(*cut)
    return level


def noise(rng, extent, width, limit, shards=(), kind=jnp.bfloat16):
    array = width * jax.random.normal(rng, extent, jnp.float32)
    if shards:
        array = array * level_of(rng, extent, shards, -0.22, 0.18)
    return jnp.clip(array, -limit, limit).astype(kind)


def setup_inputs(seed: int = 0) -> dict:
    arg_keys = jax.random.split(jax.random.key(seed), 6)
    layers = noise(arg_keys[0], (LAYERS, ROWS * SUBPIX, PCOLS), 1.0, 6.0, ((0, 4), (1, 8)))
    offsets = draw_offsets(jax.random.fold_in(arg_keys[5], 71), 0)
    subap_valid = draw_subap_valid(jax.random.fold_in(arg_keys[5], 71), 0)
    defocus = jnp.clip(jax.random.uniform(arg_keys[3], (SLICES,), jnp.float32, -0.08, 0.08), -0.08, 0.08)
    weights = jnp.clip(jnp.exp(jax.random.uniform(arg_keys[4], (SLICES,), jnp.float32, math.log(0.25), math.log(1.0))), 0.25, 1.0)
    return dict(layers=layers, offsets=offsets, subap_valid=subap_valid, defocus=defocus, weights=weights)


def tables():
    frequency = jnp.arange(SPOT, dtype=jnp.float32) - SPOT // 2
    position = jnp.arange(SUBPIX, dtype=jnp.float32) - (SUBPIX - 1) / 2.0
    phase_angle = -2.0 * math.pi / (OVER * SUBPIX) * frequency[:, None] * position[None, :]
    factor = 1.0 / math.sqrt(SUBPIX)
    real_part = jnp.cos(phase_angle) * factor
    imag_part = jnp.sin(phase_angle) * factor
    left_table = jnp.concatenate([jnp.concatenate([real_part, -imag_part], 1), jnp.concatenate([imag_part, real_part], 1)], 0).astype(jnp.bfloat16)
    right_table = jnp.concatenate([jnp.concatenate([real_part.T, imag_part.T], 1), jnp.concatenate([-imag_part.T, real_part.T], 1)], 0).astype(jnp.bfloat16)
    return (left_table, right_table)

def interpolate(window, offset_pair):
    col_steps = offset_pair[1] // QUANT
    col_frac = (offset_pair[1] % QUANT).astype(jnp.float32) / QUANT
    row_frac = (offset_pair[0] % QUANT).astype(jnp.float32) / QUANT
    col_first = jnp.roll(window, -col_steps, axis=1)
    col_second = jnp.roll(window, -(col_steps + 1), axis=1)
    across = (1.0 - col_frac) * col_first + col_frac * col_second
    return ((1.0 - row_frac) * across[:-1] + row_frac * across[1:]).astype(jnp.bfloat16)

def spots_row(pupil_phase, first_row, total_rows, defocus, weights, valid_row):
    left_table, right_table = tables()
    row_position = ((first_row + jnp.arange(SUBPIX, dtype=jnp.int32)).astype(jnp.float32) - (total_rows - 1) / 2.0) / SUBPIX
    col_position = (jnp.arange(PCOLS, dtype=jnp.float32) - (PCOLS - 1) / 2.0) / SUBPIX
    radius = row_position[:, None] ** 2 + col_position[None, :] ** 2
    spot_sum = jnp.zeros((SPOT * SUBX, SPOT), jnp.float32)
    for altitude in range(SLICES):
        phase_angle = pupil_phase + defocus[altitude] * radius
        pupil_field = jnp.concatenate([jnp.cos(phase_angle), jnp.sin(phase_angle)], 0).astype(jnp.bfloat16)
        focal_plane = jnp.dot(left_table, pupil_field, preferred_element_type=jnp.float32).astype(jnp.bfloat16)
        blocks = jnp.concatenate([focal_plane[:SPOT].reshape(SPOT * SUBX, SUBPIX), focal_plane[SPOT:].reshape(SPOT * SUBX, SUBPIX)], 1)
        spot_field = jnp.dot(blocks, right_table, preferred_element_type=jnp.float32)
        spot_sum = spot_sum + weights[altitude] * (spot_field[:, :SPOT] ** 2 + spot_field[:, SPOT:] ** 2)
    scaled = spot_sum / jnp.sum(weights)
    masked = scaled.reshape(SPOT, SUBX, SPOT) * valid_row.astype(jnp.float32)[None, :, None]
    return masked.reshape(SPOT, SUBX * SPOT).astype(jnp.bfloat16)

def reference(layers, offsets, subap_valid, defocus, weights):
    total_rows = ROWS * SUBPIX

    def one_direction(direction):
        offset_pairs = offsets[direction]

        def one_row(row_index):
            pupil_phase = jnp.zeros((SUBPIX, PCOLS), jnp.float32)
            for layer_index in range(LAYERS):
                offset_pair = offset_pairs[layer_index]
                start_row = row_index * SUBPIX + offset_pair[0] // QUANT
                rows_index = ((start_row + jnp.arange(SUBPIX + 1, dtype=jnp.int32)) % total_rows).astype(jnp.int32)
                window = jnp.take(layers[layer_index], rows_index, axis=0).astype(jnp.float32)
                pupil_phase = pupil_phase + interpolate(window, offset_pair).astype(jnp.float32)
            return spots_row(pupil_phase, row_index * SUBPIX, total_rows, defocus, weights, subap_valid[row_index])
        return lax.map(one_row, jnp.arange(ROWS, dtype=jnp.int32))
    return lax.map(one_direction, jnp.arange(DIRS, dtype=jnp.int32))
```

```python
import functools
import math

import jax
import jax.numpy as jnp
import numpy as np
from jax import lax
from jax.experimental import pallas as pl
from jax.experimental.pallas import tpu as pltpu
from jax.sharding import PartitionSpec as P

OVER = 2
QUANT = 4
REACH = 2
LANES = 128
CHUNKS = 8
MESH = pl.DeviceIdType.MESH
HALF_PI_HI = 1.5703125
HALF_PI_LO = math.pi / 2 - 1.5703125


def base_tables(n):
    frequency = np.arange(n, dtype=np.float64) - n // 2
    position = np.arange(n, dtype=np.float64) - (n - 1) / 2.0
    angle = -2.0 * math.pi / (OVER * n) * frequency[:, None] * position[None, :]
    factor = 1.0 / math.sqrt(n)
    return (np.cos(angle) * factor).astype(np.float32), (np.sin(angle) * factor).astype(np.float32)


def cos_sin(angle):
    turns = jnp.round(angle * (2.0 / math.pi))
    rest = (angle - turns * HALF_PI_HI) - turns * HALF_PI_LO
    quadrant = turns.astype(jnp.int32)
    square = rest * rest
    sin = rest + rest * square * (-1.0 / 6 + square * (1.0 / 120 - square * (1.0 / 5040)))
    cos = 1.0 + square * (-0.5 + square * (1.0 / 24 - square * (1.0 / 720 - square * (1.0 / 40320))))
    swap = (quadrant & 1) == 1
    cos_value = jnp.where(swap, sin, cos)
    sin_value = jnp.where(swap, cos, sin)
    cos_value = jnp.where(((quadrant + 1) & 2) == 2, -cos_value, cos_value)
    sin_value = jnp.where((quadrant & 2) == 2, -sin_value, sin_value)
    return cos_value, sin_value


def kernel(
    tiles, n, blocks, slices,
    x_ref, off_ref, valid_ref, defocus_ref, weights_ref, fr_ref, fi_ref, right_ref,
    out_ref,
    ext, shifted, mix, slide, send_buf, recv_buf, local, left, col_cos, col_sin,
    z_send, z_recv, s_send, s_recv, o_send, o_recv, p_send, p_recv, y_send, y_recv,
):
    tile = lax.axis_index("tile")
    own = lax.axis_index("dir")
    core = lax.rem(own, 2)
    chip = lax.div(own, 2)
    other_core = chip * 2 + (1 - core)
    other_chip = (1 - chip) * 2 + core
    odd = lax.rem(tile, 2)
    mate = tile + 1 - 2 * odd
    below = lax.rem(tile + tiles - 2, tiles)
    above = lax.rem(tile + 2, tiles)

    barrier = pltpu.get_barrier_semaphore()
    for device in ((tile, other_core), (tile, other_chip), (mate, own), (below, own), (above, own)):
        pl.semaphore_signal(barrier, inc=1, device_id=device, device_id_type=MESH)
    pl.semaphore_wait(barrier, 5)

    rows = n // CHUNKS
    pairs = blocks // 2

    def copy(source, target, send, recv, device):
        return pltpu.make_async_remote_copy(
            src_ref=source, dst_ref=target, send_sem=send, recv_sem=recv,
            device_id=device, device_id_type=MESH,
        )

    def z_copy(k):
        return copy(
            x_ref.at[0, pl.ds(k * rows, rows)], ext.at[core, 2, pl.ds(k * rows, rows)],
            z_send.at[k], z_recv.at[k], (below, own),
        )

    def first_copy(k):
        return copy(
            x_ref.at[0, pl.ds(k * rows, rows)], ext.at[core, 1, pl.ds(k * rows, rows)],
            s_send.at[k], s_recv.at[k], (mate, own),
        )

    def relay_copy(k):
        return copy(
            ext.at[core, 2, pl.ds(k * rows, rows)], ext.at[core, 1, pl.ds(k * rows, rows)],
            s_send.at[k], s_recv.at[k], (mate, own),
        )

    def share_copy(which, k):
        part = ext.at[core, which, pl.ds(k * rows, rows)]
        return copy(part, part, p_send.at[which - 1, k], p_recv.at[which - 1, k], (tile, other_core))

    own_copy = copy(x_ref.at[0], ext.at[core, 0], o_send, o_recv, (tile, other_core))

    for k in range(CHUNKS):
        z_copy(k).start()

        @pl.when(odd == 1)
        def _():
            first_copy(k).start()

    own_copy.start()
    ext[core, 0] = x_ref[0]

    first_row = (tile * n).astype(jnp.float32)
    row_at = lax.broadcasted_iota(jnp.int32, (8, n), 1).astype(jnp.float32)
    p = (first_row + row_at - (tiles * n - 1) / 2.0) / n
    col_at = lax.broadcasted_iota(jnp.int32, (8, blocks * n), 1).astype(jnp.float32)
    q = (col_at - (blocks * n - 1) / 2.0) / n
    for a in range(slices):
        row_cos, row_sin = cos_sin(defocus_ref[a] * (p * p))
        row_cos, row_sin = row_cos[0:1], row_sin[0:1]
        real = fr_ref[...] * row_cos - fi_ref[...] * row_sin
        imag = fr_ref[...] * row_sin + fi_ref[...] * row_cos
        left[2 * a * n : (2 * a + 1) * n, 0:n] = real.astype(jnp.bfloat16)
        left[2 * a * n : (2 * a + 1) * n, n : 2 * n] = (-imag).astype(jnp.bfloat16)
        left[(2 * a + 1) * n : (2 * a + 2) * n, 0:n] = imag.astype(jnp.bfloat16)
        left[(2 * a + 1) * n : (2 * a + 2) * n, n : 2 * n] = real.astype(jnp.bfloat16)
        c, s = cos_sin(defocus_ref[a] * (q * q))
        for j in range(pairs):
            col_cos[j, a] = c[:, j * 2 * n : (j + 1) * 2 * n]
            col_sin[j, a] = s[:, j * 2 * n : (j + 1) * 2 * n]

    def steps_of(direction, slot):
        return off_ref[direction, chip * 2 + slot, 0], off_ref[direction, chip * 2 + slot, 1]

    def taps(shape, shift, fraction, along, across):
        gap = lax.broadcasted_iota(jnp.int32, shape, along) - lax.broadcasted_iota(
            jnp.int32, shape, across
        ) - shift
        return jnp.where(gap == 0, 1.0 - fraction, jnp.where(gap == 1, fraction, 0.0)).astype(
            jnp.bfloat16
        )

    for index, direction in enumerate((other_chip, own)):
        for slot in range(2):
            row_steps, col_steps = steps_of(direction, slot)
            fy = (row_steps & (QUANT - 1)).astype(jnp.float32) * (1.0 / QUANT)
            fx = (col_steps & (QUANT - 1)).astype(jnp.float32) * (1.0 / QUANT)
            down = lax.shift_right_logical(row_steps, 2) & (n - 1)
            over = lax.shift_right_logical(col_steps, 2) & (n - 1)
            mix[index, slot] = taps((n, 2 * n), down, fy, 1, 0)
            tap = taps((3 * n, 2 * n), over, fx, 0, 1)
            for half in range(2):
                first = (slot * 2 + half) * 3 * n
                slide[index, first : first + 3 * n, :] = tap

    for k in range(CHUNKS):
        z_copy(k).wait_recv()
        share_copy(2, k).start()

        @pl.when(odd == 0)
        def _():
            relay_copy(k).start()

        first_copy(k).wait_recv()
        share_copy(1, k).start()
    own_copy.wait_recv()
    for k in range(CHUNKS):
        share_copy(2, k).wait_recv()
        share_copy(1, k).wait_recv()

    def interpolated(index, direction, store, after):
        plans = []
        for slot in range(2):
            row_steps, col_steps = steps_of(direction, slot)
            top = lax.shift_right_logical(row_steps, n.bit_length() + 1)
            plans.append((top, lax.shift_right_logical(col_steps, n.bit_length() + 1)))

        def rows_step(j, carry):
            span = pl.ds(pl.multiple_of(j * 2 * n, 2 * n), 2 * n)
            for slot in range(2):
                top = plans[slot][0]
                window = jnp.concatenate([ext[slot, top, :, span], ext[slot, top + 1, :, span]], 0)
                mixed = jnp.dot(mix[index, slot], window, preferred_element_type=jnp.float32)
                high = mixed.astype(jnp.bfloat16)
                low = (mixed - high.astype(jnp.float32)).astype(jnp.bfloat16)
                for b in range(2):
                    shifted[slot, 0, 2 * j + b] = high[:, b * n : (b + 1) * n]
                    shifted[slot, 1, 2 * j + b] = low[:, b * n : (b + 1) * n]
            return carry

        lax.fori_loop(0, pairs, rows_step, 0)

        def cols_step(j, carry):
            parts = []
            for slot in range(2):
                begin = plans[slot][1] + 2 * j
                for half in range(2):
                    for b in range(3):
                        parts.append(shifted[slot, half, (begin + b) & (blocks - 1)])
            total = jnp.dot(
                jnp.concatenate(parts, 1), slide[index], preferred_element_type=jnp.float32
            )
            store(j, [total[:, :n], total[:, n:]])
            after(j)
            return carry

        lax.fori_loop(0, pairs, cols_step, 0)

    def y_copy(j):
        return copy(send_buf.at[j], recv_buf.at[j], y_send.at[j], y_recv.at[j], (tile, other_chip))

    def store_send(j, total):
        for b in range(2):
            send_buf[j, b] = total[b].astype(jnp.bfloat16)

    def send_previous(j):
        @pl.when(j > 0)
        def _():
            y_copy(j - 1).start()

    def store_local(j, total):
        for b in range(2):
            local[j, b] = total[b]

        @pl.when(j == 0)
        def _():
            y_copy(pairs - 1).start()

    interpolated(0, other_chip, store_send, send_previous)
    interpolated(1, own, store_local, lambda j: None)

    weight_sum = weights_ref[0]
    for a in range(1, slices):
        weight_sum = weight_sum + weights_ref[a]

    def final_step(j, carry):
        y_copy(j).wait_recv()
        fields = []
        for b in range(2):
            c, s = cos_sin(local[j, b] + recv_buf[j, b].astype(jnp.float32))
            fields.append(jnp.concatenate([c, s], 0).astype(jnp.bfloat16))
        field = jnp.concatenate(fields, 1)
        sums = [jnp.zeros((n, n), jnp.float32) for _ in range(2)]
        for a in range(slices):
            focal = jnp.dot(
                left[2 * a * n : (2 * a + 2) * n, :], field, preferred_element_type=jnp.float32
            )
            real, imag = focal[:n], focal[n:]
            c, s = col_cos[j, a][0:1], col_sin[j, a][0:1]
            new_real = (real * c - imag * s).astype(jnp.bfloat16)
            new_imag = (real * s + imag * c).astype(jnp.bfloat16)
            both = jnp.concatenate(
                [
                    jnp.concatenate([new_real[:, b * n : (b + 1) * n], new_imag[:, b * n : (b + 1) * n]], 1)
                    for b in range(2)
                ],
                0,
            )
            spot = jnp.dot(both, right_ref[...], preferred_element_type=jnp.float32)
            power = spot * spot
            for b in range(2):
                piece = power[b * n : (b + 1) * n]
                sums[b] = sums[b] + weights_ref[a] * (piece[:, :n] + piece[:, n:])
        for b in range(2):
            lit = valid_ref[0, 2 * j + b].astype(jnp.float32)
            out_ref[0, 0, :, pl.ds(pl.multiple_of((2 * j + b) * n, n), n)] = (
                sums[b] / weight_sum * lit
            ).astype(jnp.bfloat16)
        return carry

    lax.fori_loop(0, pairs, final_step, 0)

    for k in range(CHUNKS):
        z_copy(k).wait_send()
        first_copy(k).wait_send()
        share_copy(1, k).wait_send()
        share_copy(2, k).wait_send()
    own_copy.wait_send()
    for j in range(pairs):
        y_copy(j).wait_send()


def solution(mesh):
    tiles = mesh.shape["tile"]

    def shards(layers, offsets, subap_valid, defocus, weights):
        n, cols = layers.shape[1], layers.shape[2]
        blocks = cols // n
        slices = defocus.shape[0]
        pairs = blocks // 2
        fr, fi = base_tables(n)
        right = jnp.asarray(np.block([[fr.T, fi.T], [-fi.T, fr.T]])).astype(jnp.bfloat16)
        vmem = pl.BlockSpec(memory_space=pltpu.VMEM)
        smem = pl.BlockSpec(memory_space=pltpu.SMEM)
        dma = pltpu.SemaphoreType.DMA
        return pl.pallas_call(
            functools.partial(kernel, tiles, n, blocks, slices),
            out_shape=jax.ShapeDtypeStruct((1, 1, n, cols), jnp.bfloat16),
            in_specs=[vmem, smem, smem, smem, smem, vmem, vmem, vmem],
            out_specs=vmem,
            scratch_shapes=[
                pltpu.VMEM((2, REACH + 1, n, cols), jnp.bfloat16),
                pltpu.VMEM((2, 2, blocks, n, n), jnp.bfloat16),
                pltpu.VMEM((2, 2, n, 2 * n), jnp.bfloat16),
                pltpu.VMEM((2, 12 * n, 2 * n), jnp.bfloat16),
                pltpu.VMEM((pairs, 2, n, n), jnp.bfloat16),
                pltpu.VMEM((pairs, 2, n, n), jnp.bfloat16),
                pltpu.VMEM((pairs, 2, n, n), jnp.float32),
                pltpu.VMEM((2 * slices * n, 2 * n), jnp.bfloat16),
                pltpu.VMEM((pairs, slices, 8, 2 * n), jnp.float32),
                pltpu.VMEM((pairs, slices, 8, 2 * n), jnp.float32),
                dma((CHUNKS,)), dma((CHUNKS,)),
                dma((CHUNKS,)), dma((CHUNKS,)),
                dma, dma,
                dma((REACH, CHUNKS)), dma((REACH, CHUNKS)),
                dma((pairs,)), dma((pairs,)),
            ],
            compiler_params=pltpu.CompilerParams(collective_id=0, has_side_effects=True),
        )(layers, offsets, subap_valid, defocus, weights, jnp.asarray(fr), jnp.asarray(fi), right)

    placed = (P("dir", "tile", None), P(), P("tile", None), P(), P())
    return jax.shard_map(
        shards, mesh=mesh, in_specs=placed, out_specs=P("dir", "tile", None, None), check_vma=False
    )
```

```python
import functools
import math

import jax
import jax.numpy as jnp
import numpy as np
from jax import lax
from jax.experimental import pallas as pl
from jax.experimental.pallas import tpu as pltpu
from jax.sharding import PartitionSpec as P

OVER = 2
QUANT = 4
REACH = 2
LANES = 128
CHUNKS = 8
MESH = pl.DeviceIdType.MESH
HALF_PI_HI = 1.5703125
HALF_PI_LO = math.pi / 2 - 1.5703125


def base_tables(n):
    frequency = np.arange(n, dtype=np.float64) - n // 2
    position = np.arange(n, dtype=np.float64) - (n - 1) / 2.0
    angle = -2.0 * math.pi / (OVER * n) * frequency[:, None] * position[None, :]
    factor = 1.0 / math.sqrt(n)
    return (np.cos(angle) * factor).astype(np.float32), (np.sin(angle) * factor).astype(np.float32)


def cos_sin(angle):
    turns = jnp.round(angle * (2.0 / math.pi))
    rest = (angle - turns * HALF_PI_HI) - turns * HALF_PI_LO
    quadrant = turns.astype(jnp.int32)
    square = rest * rest
    sin = rest + rest * square * (-1.0 / 6 + square * (1.0 / 120 - square * (1.0 / 5040)))
    cos = 1.0 + square * (-0.5 + square * (1.0 / 24 - square * (1.0 / 720 - square * (1.0 / 40320))))
    swap = (quadrant & 1) == 1
    cos_value = jnp.where(swap, sin, cos)
    sin_value = jnp.where(swap, cos, sin)
    cos_value = jnp.where(((quadrant + 1) & 2) == 2, -cos_value, cos_value)
    sin_value = jnp.where((quadrant & 2) == 2, -sin_value, sin_value)
    return cos_value, sin_value


def kernel(
    tiles, n, blocks, slices,
    x_ref, off_ref, valid_ref, defocus_ref, weights_ref, fr_ref, fi_ref, right_ref,
    out_ref,
    ext_a, ext_b, ext_far, shifted, mix, slide, send_buf, recv_buf, local, left, col_cos, col_sin,
    z_send, z_recv, s_send, s_recv, o_send, o_recv, r_send, r_recv, p_send, p_recv, y_send, y_recv,
):
    tile = lax.axis_index("tile")
    own = lax.axis_index("dir")
    core = lax.rem(own, 2)
    chip = lax.div(own, 2)
    other_core = chip * 2 + (1 - core)
    other_chip = (1 - chip) * 2 + core
    odd = lax.rem(tile, 2)
    mate = tile + 1 - 2 * odd
    below = lax.rem(tile + tiles - 2, tiles)
    above = lax.rem(tile + 2, tiles)

    barrier = pltpu.get_barrier_semaphore()
    for device in ((tile, other_core), (tile, other_chip), (mate, own), (below, own), (above, own)):
        pl.semaphore_signal(barrier, inc=1, device_id=device, device_id_type=MESH)
    pl.semaphore_wait(barrier, 5)

    ext = (ext_a, ext_b, ext_far)
    rows = n // CHUNKS
    pairs = blocks // 2

    def copy(source, target, send, recv, device):
        return pltpu.make_async_remote_copy(
            src_ref=source, dst_ref=target, send_sem=send, recv_sem=recv,
            device_id=device, device_id_type=MESH,
        )

    def part(slot, which, k):
        return ext[slot].at[which, pl.ds(k * rows, rows)]

    def source(slot, k):
        return part(2, 0, k) if slot == 2 else x_ref.at[0, pl.ds(k * rows, rows)]

    def z_copy(slot, k):
        return copy(
            source(slot, k), part(slot, 2, k), z_send.at[slot, k], z_recv.at[slot, k], (below, own)
        )

    def first_copy(slot, k):
        return copy(
            source(slot, k), part(slot, 1, k), s_send.at[slot, k], s_recv.at[slot, k], (mate, own)
        )

    def relay_copy(slot, k):
        return copy(
            part(slot, 2, k), part(slot, 1, k), s_send.at[slot, k], s_recv.at[slot, k], (mate, own)
        )

    def raw_copy(k):
        return copy(
            x_ref.at[0, pl.ds(k * rows, rows)], part(2, 0, k), r_send.at[k], r_recv.at[k],
            (tile, other_chip),
        )

    def share_copy(slot, which, k):
        return copy(
            part(slot, which, k), part(slot, which, k),
            p_send.at[slot, which, k], p_recv.at[slot, which, k], (tile, other_core),
        )

    def own_copy(slot):
        return copy(x_ref.at[0], ext[slot].at[0], o_send.at[slot], o_recv.at[slot], (tile, other_core))

    def send_halo(slot, k):
        z_copy(slot, k).start()

        @pl.when(odd == 1)
        def _():
            first_copy(slot, k).start()

    def pass_on(slot, k):
        z_copy(slot, k).wait_recv()

        @pl.when(odd == 0)
        def _():
            relay_copy(slot, k).start()

        share_copy(slot, 2, k).start()
        first_copy(slot, k).wait_recv()
        share_copy(slot, 1, k).start()

    def take(slot, k):
        share_copy(slot, 2, k).wait_recv()
        share_copy(slot, 1, k).wait_recv()

    @pl.when(core == 0)
    def _():
        for k in range(CHUNKS):
            send_halo(0, k)
        own_copy(0).start()
        ext_a[0] = x_ref[0]

    @pl.when(core == 1)
    def _():
        for k in range(CHUNKS):
            raw_copy(k).start()
        own_copy(1).start()
        ext_b[0] = x_ref[0]

    first_row = (tile * n).astype(jnp.float32)
    row_at = lax.broadcasted_iota(jnp.int32, (8, n), 1).astype(jnp.float32)
    p = (first_row + row_at - (tiles * n - 1) / 2.0) / n
    col_at = lax.broadcasted_iota(jnp.int32, (8, blocks * n), 1).astype(jnp.float32)
    q = (col_at - (blocks * n - 1) / 2.0) / n
    for a in range(slices):
        row_cos, row_sin = cos_sin(defocus_ref[a] * (p * p))
        row_cos, row_sin = row_cos[0:1], row_sin[0:1]
        real = fr_ref[...] * row_cos - fi_ref[...] * row_sin
        imag = fr_ref[...] * row_sin + fi_ref[...] * row_cos
        left[2 * a * n : (2 * a + 1) * n, 0:n] = real.astype(jnp.bfloat16)
        left[2 * a * n : (2 * a + 1) * n, n : 2 * n] = (-imag).astype(jnp.bfloat16)
        left[(2 * a + 1) * n : (2 * a + 2) * n, 0:n] = imag.astype(jnp.bfloat16)
        left[(2 * a + 1) * n : (2 * a + 2) * n, n : 2 * n] = real.astype(jnp.bfloat16)
        c, s = cos_sin(defocus_ref[a] * (q * q))
        for j in range(pairs):
            col_cos[j, a] = c[:, j * 2 * n : (j + 1) * 2 * n]
            col_sin[j, a] = s[:, j * 2 * n : (j + 1) * 2 * n]

    def taps(shape, shift, fraction, along, across):
        gap = lax.broadcasted_iota(jnp.int32, shape, along) - lax.broadcasted_iota(
            jnp.int32, shape, across
        ) - shift
        return jnp.where(gap == 0, 1.0 - fraction, jnp.where(gap == 1, fraction, 0.0)).astype(
            jnp.bfloat16
        )

    layer_a, layer_b, layer_far = chip * 2, chip * 2 + 1, (1 - chip) * 2 + 1
    terms = ((other_chip, layer_a), (own, layer_a), (own, layer_b), (own, layer_far))
    slots = (0, 0, 1, 2)
    tops, begins = [], []
    for term, (direction, layer) in enumerate(terms):
        row_steps, col_steps = off_ref[direction, 0, layer], off_ref[direction, 1, layer]
        tops.append(lax.shift_right_logical(row_steps, n.bit_length() + 1))
        begins.append(lax.shift_right_logical(col_steps, n.bit_length() + 1))
        fy = (row_steps & (QUANT - 1)).astype(jnp.float32) * (1.0 / QUANT)
        fx = (col_steps & (QUANT - 1)).astype(jnp.float32) * (1.0 / QUANT)
        down = lax.shift_right_logical(row_steps, 2) & (n - 1)
        over = lax.shift_right_logical(col_steps, 2) & (n - 1)
        mix[term] = taps((n, 2 * n), down, fy, 1, 0)
        tap = taps((3 * n, 2 * n), over, fx, 0, 1)
        slide[6 * term * n : (6 * term + 3) * n, :] = tap
        slide[(6 * term + 3) * n : (6 * term + 6) * n, :] = tap

    def rows_step(term, j):
        span = pl.ds(pl.multiple_of(j * 2 * n, 2 * n), 2 * n)
        slot, top = slots[term], tops[term]
        window = jnp.concatenate([ext[slot][top, :, span], ext[slot][top + 1, :, span]], 0)
        mixed = jnp.dot(mix[term], window, preferred_element_type=jnp.float32)
        high = mixed.astype(jnp.bfloat16)
        low = (mixed - high.astype(jnp.float32)).astype(jnp.bfloat16)
        for b in range(2):
            shifted[term, 0, 2 * j + b] = high[:, b * n : (b + 1) * n]
            shifted[term, 1, 2 * j + b] = low[:, b * n : (b + 1) * n]

    def cols_step(first, last, j):
        parts = []
        for term in range(first, last):
            begin = begins[term] + 2 * j
            for half in range(2):
                for b in range(3):
                    parts.append(shifted[term, half, (begin + b) & (blocks - 1)])
        return jnp.dot(
            jnp.concatenate(parts, 1), slide[6 * first * n : 6 * last * n, :],
            preferred_element_type=jnp.float32,
        )

    def y_copy(j):
        return copy(send_buf.at[j], recv_buf.at[j], y_send.at[j], y_recv.at[j], (tile, other_chip))

    def loop(body):
        def step(j, carry):
            body(j)
            return carry

        lax.fori_loop(0, pairs, step, 0)

    @pl.when(core == 0)
    def _():
        loop(lambda k: pass_on(0, k))

    @pl.when(core == 1)
    def _():
        own_copy(0).wait_recv()
        for k in range(CHUNKS // 2):
            take(0, k)
        for k in range(CHUNKS):
            send_halo(1, k)
        for k in range(CHUNKS):
            raw_copy(k).wait_recv()
            share_copy(2, 0, k).start()
            send_halo(2, k)
        for k in range(CHUNKS // 2, CHUNKS):
            take(0, k)

    loop(lambda j: rows_step(0, j))

    def send_step(j):
        send_buf[j] = cols_step(0, 1, j).astype(jnp.bfloat16)

        @pl.when(j > 0)
        def _():
            y_copy(j - 1).start()

    loop(send_step)

    def near_step(j):
        rows_step(1, j)

        @pl.when(j == 0)
        def _():
            y_copy(pairs - 1).start()

        @pl.when(core == 0)
        def _():
            take(1, j)

        @pl.when(core == 1)
        def _():
            pass_on(1, j)

    loop(near_step)

    @pl.when(core == 0)
    def _():
        own_copy(1).wait_recv()

    def far_step(j):
        rows_step(2, j)
        local[j] = cols_step(1, 2, j)

        @pl.when(core == 0)
        def _():
            share_copy(2, 0, j).wait_recv()
            take(2, j)

        @pl.when(core == 1)
        def _():
            pass_on(2, j)

    loop(far_step)
    loop(lambda j: rows_step(3, j))

    weight_sum = weights_ref[0]
    for a in range(1, slices):
        weight_sum = weight_sum + weights_ref[a]

    def final_step(j, carry):
        y_copy(j).wait_recv()
        phase = local[j] + cols_step(2, 4, j) + recv_buf[j].astype(jnp.float32)
        field = jnp.concatenate(cos_sin(phase), 0).astype(jnp.bfloat16)
        sums = [jnp.zeros((n, n), jnp.float32) for _ in range(2)]
        for a in range(slices):
            focal = jnp.dot(
                left[2 * a * n : (2 * a + 2) * n, :], field, preferred_element_type=jnp.float32
            )
            real, imag = focal[:n], focal[n:]
            c, s = col_cos[j, a][0:1], col_sin[j, a][0:1]
            new_real = (real * c - imag * s).astype(jnp.bfloat16)
            new_imag = (real * s + imag * c).astype(jnp.bfloat16)
            both = jnp.concatenate(
                [
                    jnp.concatenate([new_real[:, b * n : (b + 1) * n], new_imag[:, b * n : (b + 1) * n]], 1)
                    for b in range(2)
                ],
                0,
            )
            spot = jnp.dot(both, right_ref[...], preferred_element_type=jnp.float32)
            power = spot * spot
            for b in range(2):
                piece = power[b * n : (b + 1) * n]
                sums[b] = sums[b] + weights_ref[a] * (piece[:, :n] + piece[:, n:])
        for b in range(2):
            lit = valid_ref[0, 2 * j + b].astype(jnp.float32)
            out_ref[0, 0, :, pl.ds(pl.multiple_of((2 * j + b) * n, n), n)] = (
                sums[b] / weight_sum * lit
            ).astype(jnp.bfloat16)
        return carry

    lax.fori_loop(0, pairs, final_step, 0)

    def finish(slot):
        own_copy(slot).wait_send() if slot < 2 else None
        for k in range(CHUNKS):
            z_copy(slot, k).wait_send()
            first_copy(slot, k).wait_send()
            share_copy(slot, 1, k).wait_send()
            share_copy(slot, 2, k).wait_send()
            if slot == 2:
                share_copy(slot, 0, k).wait_send()
                raw_copy(k).wait_send()

    @pl.when(core == 0)
    def _():
        finish(0)

    @pl.when(core == 1)
    def _():
        finish(1)
        finish(2)

    for j in range(pairs):
        y_copy(j).wait_send()


def solution(mesh):
    tiles = mesh.shape["tile"]

    def shards(layers, offsets, subap_valid, defocus, weights):
        n, cols = layers.shape[1], layers.shape[2]
        blocks = cols // n
        slices = defocus.shape[0]
        pairs = blocks // 2
        fr, fi = base_tables(n)
        right = jnp.asarray(np.block([[fr.T, fi.T], [-fi.T, fr.T]])).astype(jnp.bfloat16)
        vmem = pl.BlockSpec(memory_space=pltpu.VMEM)
        smem = pl.BlockSpec(memory_space=pltpu.SMEM)
        dma = pltpu.SemaphoreType.DMA
        return pl.pallas_call(
            functools.partial(kernel, tiles, n, blocks, slices),
            out_shape=jax.ShapeDtypeStruct((1, 1, n, cols), jnp.bfloat16),
            in_specs=[vmem, smem, smem, smem, smem, vmem, vmem, vmem],
            out_specs=vmem,
            scratch_shapes=[
                pltpu.VMEM((REACH + 1, n, cols), jnp.bfloat16),
                pltpu.VMEM((REACH + 1, n, cols), jnp.bfloat16),
                pltpu.VMEM((REACH + 1, n, cols), jnp.bfloat16),
                pltpu.VMEM((4, 2, blocks, n, n), jnp.bfloat16),
                pltpu.VMEM((4, n, 2 * n), jnp.bfloat16),
                pltpu.VMEM((24 * n, 2 * n), jnp.bfloat16),
                pltpu.VMEM((pairs, n, 2 * n), jnp.bfloat16),
                pltpu.VMEM((pairs, n, 2 * n), jnp.bfloat16),
                pltpu.VMEM((pairs, n, 2 * n), jnp.float32),
                pltpu.VMEM((2 * slices * n, 2 * n), jnp.bfloat16),
                pltpu.VMEM((pairs, slices, 8, 2 * n), jnp.float32),
                pltpu.VMEM((pairs, slices, 8, 2 * n), jnp.float32),
                dma((3, CHUNKS)), dma((3, CHUNKS)),
                dma((3, CHUNKS)), dma((3, CHUNKS)),
                dma((2,)), dma((2,)),
                dma((CHUNKS,)), dma((CHUNKS,)),
                dma((3, REACH + 1, CHUNKS)), dma((3, REACH + 1, CHUNKS)),
                dma((pairs,)), dma((pairs,)),
            ],
            compiler_params=pltpu.CompilerParams(collective_id=0, has_side_effects=True),
        )(layers, jnp.transpose(offsets, (0, 2, 1)), subap_valid, defocus, weights, jnp.asarray(fr), jnp.asarray(fi), right)

    placed = (P("dir", "tile", None), P(), P("tile", None), P(), P())
    return jax.shard_map(
        shards, mesh=mesh, in_specs=placed, out_specs=P("dir", "tile", None, None), check_vma=False
    )
```

```python
import functools
import math

import jax
import jax.numpy as jnp
import numpy as np
from jax import lax
from jax.experimental import pallas as pl
from jax.experimental.pallas import tpu as pltpu
from jax.sharding import PartitionSpec as P

OVER = 2
QUANT = 4
REACH = 2
LANES = 128
CHUNKS = 8
MESH = pl.DeviceIdType.MESH
HALF_PI_HI = 1.5703125
HALF_PI_LO = math.pi / 2 - 1.5703125


def base_tables(n):
    frequency = np.arange(n, dtype=np.float64) - n // 2
    position = np.arange(n, dtype=np.float64) - (n - 1) / 2.0
    angle = -2.0 * math.pi / (OVER * n) * frequency[:, None] * position[None, :]
    factor = 1.0 / math.sqrt(n)
    return (np.cos(angle) * factor).astype(np.float32), (np.sin(angle) * factor).astype(np.float32)


def cos_sin(angle):
    turns = jnp.round(angle * (2.0 / math.pi))
    rest = (angle - turns * HALF_PI_HI) - turns * HALF_PI_LO
    quadrant = turns.astype(jnp.int32)
    square = rest * rest
    sin = rest + rest * square * (-1.0 / 6 + square * (1.0 / 120 - square * (1.0 / 5040)))
    cos = 1.0 + square * (-0.5 + square * (1.0 / 24 - square * (1.0 / 720 - square * (1.0 / 40320))))
    swap = (quadrant & 1) == 1
    cos_value = jnp.where(swap, sin, cos)
    sin_value = jnp.where(swap, cos, sin)
    cos_value = jnp.where(((quadrant + 1) & 2) == 2, -cos_value, cos_value)
    sin_value = jnp.where((quadrant & 2) == 2, -sin_value, sin_value)
    return cos_value, sin_value


def kernel(
    tiles, n, blocks, slices,
    x_ref, off_ref, valid_ref, defocus_ref, weights_ref, fr_ref, fi_ref, right_ref,
    out_ref,
    ext, shifted, mix, slide, send_buf, recv_buf, local, left, col_cos, col_sin,
    z_send, z_recv, s_send, s_recv, o_send, o_recv, p_send, p_recv, y_send, y_recv,
):
    tile = lax.axis_index("tile")
    own = lax.axis_index("dir")
    core = lax.rem(own, 2)
    chip = lax.div(own, 2)
    other_core = chip * 2 + (1 - core)
    other_chip = (1 - chip) * 2 + core
    odd = lax.rem(tile, 2)
    mate = tile + 1 - 2 * odd
    below = lax.rem(tile + tiles - 2, tiles)
    above = lax.rem(tile + 2, tiles)

    barrier = pltpu.get_barrier_semaphore()
    for device in ((tile, other_core), (tile, other_chip), (mate, own), (below, own), (above, own)):
        pl.semaphore_signal(barrier, inc=1, device_id=device, device_id_type=MESH)
    pl.semaphore_wait(barrier, 5)

    rows = n // CHUNKS
    pairs = blocks // 2

    def copy(source, target, send, recv, device):
        return pltpu.make_async_remote_copy(
            src_ref=source, dst_ref=target, send_sem=send, recv_sem=recv,
            device_id=device, device_id_type=MESH,
        )

    def z_copy(k):
        return copy(
            x_ref.at[0, pl.ds(k * rows, rows)], ext.at[core, 2, pl.ds(k * rows, rows)],
            z_send.at[k], z_recv.at[k], (below, own),
        )

    def first_copy(k):
        return copy(
            x_ref.at[0, pl.ds(k * rows, rows)], ext.at[core, 1, pl.ds(k * rows, rows)],
            s_send.at[k], s_recv.at[k], (mate, own),
        )

    def relay_copy(k):
        return copy(
            ext.at[core, 2, pl.ds(k * rows, rows)], ext.at[core, 1, pl.ds(k * rows, rows)],
            s_send.at[k], s_recv.at[k], (mate, own),
        )

    def share_copy(which, k):
        part = ext.at[core, which, pl.ds(k * rows, rows)]
        return copy(part, part, p_send.at[which - 1, k], p_recv.at[which - 1, k], (tile, other_core))

    own_copy = copy(x_ref.at[0], ext.at[core, 0], o_send, o_recv, (tile, other_core))

    for k in range(CHUNKS):
        z_copy(k).start()

        @pl.when(odd == 1)
        def _():
            first_copy(k).start()

    own_copy.start()
    ext[core, 0] = x_ref[0]

    first_row = (tile * n).astype(jnp.float32)
    row_at = lax.broadcasted_iota(jnp.int32, (8, n), 1).astype(jnp.float32)
    p = (first_row + row_at - (tiles * n - 1) / 2.0) / n
    col_at = lax.broadcasted_iota(jnp.int32, (8, blocks * n), 1).astype(jnp.float32)
    q = (col_at - (blocks * n - 1) / 2.0) / n
    for a in range(slices):
        row_cos, row_sin = cos_sin(defocus_ref[a] * (p * p))
        row_cos, row_sin = row_cos[0:1], row_sin[0:1]
        real = fr_ref[...] * row_cos - fi_ref[...] * row_sin
        imag = fr_ref[...] * row_sin + fi_ref[...] * row_cos
        left[2 * a * n : (2 * a + 1) * n, 0:n] = real.astype(jnp.bfloat16)
        left[2 * a * n : (2 * a + 1) * n, n : 2 * n] = (-imag).astype(jnp.bfloat16)
        left[(2 * a + 1) * n : (2 * a + 2) * n, 0:n] = imag.astype(jnp.bfloat16)
        left[(2 * a + 1) * n : (2 * a + 2) * n, n : 2 * n] = real.astype(jnp.bfloat16)
        c, s = cos_sin(defocus_ref[a] * (q * q))
        for j in range(pairs):
            col_cos[j, a] = c[:, j * 2 * n : (j + 1) * 2 * n]
            col_sin[j, a] = s[:, j * 2 * n : (j + 1) * 2 * n]

    def steps_of(direction, slot):
        return off_ref[direction, 0, chip * 2 + slot], off_ref[direction, 1, chip * 2 + slot]

    def taps(shape, shift, fraction, along, across):
        gap = lax.broadcasted_iota(jnp.int32, shape, along) - lax.broadcasted_iota(
            jnp.int32, shape, across
        ) - shift
        return jnp.where(gap == 0, 1.0 - fraction, jnp.where(gap == 1, fraction, 0.0)).astype(
            jnp.bfloat16
        )

    for index, direction in enumerate((other_chip, own)):
        for slot in range(2):
            row_steps, col_steps = steps_of(direction, slot)
            fy = (row_steps & (QUANT - 1)).astype(jnp.float32) * (1.0 / QUANT)
            fx = (col_steps & (QUANT - 1)).astype(jnp.float32) * (1.0 / QUANT)
            down = lax.shift_right_logical(row_steps, 2) & (n - 1)
            over = lax.shift_right_logical(col_steps, 2) & (n - 1)
            mix[index, slot] = taps((n, 2 * n), down, fy, 1, 0)
            tap = taps((3 * n, 2 * n), over, fx, 0, 1)
            for half in range(2):
                first = (slot * 2 + half) * 3 * n
                slide[index, first : first + 3 * n, :] = tap

    for k in range(CHUNKS):
        z_copy(k).wait_recv()
        share_copy(2, k).start()

        @pl.when(odd == 0)
        def _():
            relay_copy(k).start()

        first_copy(k).wait_recv()
        share_copy(1, k).start()
    own_copy.wait_recv()
    for k in range(CHUNKS):
        share_copy(2, k).wait_recv()
        share_copy(1, k).wait_recv()

    def interpolated(index, direction, store, after):
        plans = []
        for slot in range(2):
            row_steps, col_steps = steps_of(direction, slot)
            top = lax.shift_right_logical(row_steps, n.bit_length() + 1)
            plans.append((top, lax.shift_right_logical(col_steps, n.bit_length() + 1)))

        def rows_step(j, carry):
            span = pl.ds(pl.multiple_of(j * 2 * n, 2 * n), 2 * n)
            for slot in range(2):
                top = plans[slot][0]
                window = jnp.concatenate([ext[slot, top, :, span], ext[slot, top + 1, :, span]], 0)
                mixed = jnp.dot(mix[index, slot], window, preferred_element_type=jnp.float32)
                high = mixed.astype(jnp.bfloat16)
                low = (mixed - high.astype(jnp.float32)).astype(jnp.bfloat16)
                for b in range(2):
                    shifted[slot, 0, 2 * j + b] = high[:, b * n : (b + 1) * n]
                    shifted[slot, 1, 2 * j + b] = low[:, b * n : (b + 1) * n]
            return carry

        lax.fori_loop(0, pairs, rows_step, 0, unroll=4)

        def cols_step(j, carry):
            parts = []
            for slot in range(2):
                begin = plans[slot][1] + 2 * j
                for half in range(2):
                    for b in range(3):
                        parts.append(shifted[slot, half, (begin + b) & (blocks - 1)])
            total = jnp.dot(
                jnp.concatenate(parts, 1), slide[index], preferred_element_type=jnp.float32
            )
            store(j, [total[:, :n], total[:, n:]])
            after(j)
            return carry

        lax.fori_loop(0, pairs, cols_step, 0, unroll=2)

    def y_copy(j):
        return copy(send_buf.at[j], recv_buf.at[j], y_send.at[j], y_recv.at[j], (tile, other_chip))

    def store_send(j, total):
        for b in range(2):
            send_buf[j, b] = total[b].astype(jnp.bfloat16)

    def send_previous(j):
        @pl.when(j > 0)
        def _():
            y_copy(j - 1).start()

    def store_local(j, total):
        for b in range(2):
            local[j, b] = total[b]

        @pl.when(j == 0)
        def _():
            y_copy(pairs - 1).start()

    interpolated(0, other_chip, store_send, send_previous)
    interpolated(1, own, store_local, lambda j: None)

    weight_sum = weights_ref[0]
    for a in range(1, slices):
        weight_sum = weight_sum + weights_ref[a]

    def final_step(j, carry):
        y_copy(j).wait_recv()
        fields = []
        for b in range(2):
            c, s = cos_sin(local[j, b] + recv_buf[j, b].astype(jnp.float32))
            fields.append(jnp.concatenate([c, s], 0).astype(jnp.bfloat16))
        field = jnp.concatenate(fields, 1)
        sums = [jnp.zeros((n, n), jnp.float32) for _ in range(2)]
        for a in range(slices):
            focal = jnp.dot(
                left[2 * a * n : (2 * a + 2) * n, :], field, preferred_element_type=jnp.float32
            )
            real, imag = focal[:n], focal[n:]
            c, s = col_cos[j, a][0:1], col_sin[j, a][0:1]
            new_real = (real * c - imag * s).astype(jnp.bfloat16)
            new_imag = (real * s + imag * c).astype(jnp.bfloat16)
            both = jnp.concatenate(
                [
                    jnp.concatenate([new_real[:, b * n : (b + 1) * n], new_imag[:, b * n : (b + 1) * n]], 1)
                    for b in range(2)
                ],
                0,
            )
            spot = jnp.dot(both, right_ref[...], preferred_element_type=jnp.float32)
            power = spot * spot
            for b in range(2):
                piece = power[b * n : (b + 1) * n]
                sums[b] = sums[b] + weights_ref[a] * (piece[:, :n] + piece[:, n:])
        for b in range(2):
            lit = valid_ref[0, 2 * j + b].astype(jnp.float32)
            out_ref[0, 0, :, pl.ds(pl.multiple_of((2 * j + b) * n, n), n)] = (
                sums[b] / weight_sum * lit
            ).astype(jnp.bfloat16)
        return carry

    lax.fori_loop(0, pairs, final_step, 0, unroll=2)

    for k in range(CHUNKS):
        z_copy(k).wait_send()
        first_copy(k).wait_send()
        share_copy(1, k).wait_send()
        share_copy(2, k).wait_send()
    own_copy.wait_send()
    for j in range(pairs):
        y_copy(j).wait_send()


def solution(mesh):
    tiles = mesh.shape["tile"]

    def shards(layers, offsets, subap_valid, defocus, weights):
        n, cols = layers.shape[1], layers.shape[2]
        blocks = cols // n
        slices = defocus.shape[0]
        pairs = blocks // 2
        fr, fi = base_tables(n)
        right = jnp.asarray(np.block([[fr.T, fi.T], [-fi.T, fr.T]])).astype(jnp.bfloat16)
        vmem = pl.BlockSpec(memory_space=pltpu.VMEM)
        smem = pl.BlockSpec(memory_space=pltpu.SMEM)
        dma = pltpu.SemaphoreType.DMA
        return pl.pallas_call(
            functools.partial(kernel, tiles, n, blocks, slices),
            out_shape=jax.ShapeDtypeStruct((1, 1, n, cols), jnp.bfloat16),
            in_specs=[vmem, smem, smem, smem, smem, vmem, vmem, vmem],
            out_specs=vmem,
            scratch_shapes=[
                pltpu.VMEM((2, REACH + 1, n, cols), jnp.bfloat16),
                pltpu.VMEM((2, 2, blocks, n, n), jnp.bfloat16),
                pltpu.VMEM((2, 2, n, 2 * n), jnp.bfloat16),
                pltpu.VMEM((2, 12 * n, 2 * n), jnp.bfloat16),
                pltpu.VMEM((pairs, 2, n, n), jnp.bfloat16),
                pltpu.VMEM((pairs, 2, n, n), jnp.bfloat16),
                pltpu.VMEM((pairs, 2, n, n), jnp.float32),
                pltpu.VMEM((2 * slices * n, 2 * n), jnp.bfloat16),
                pltpu.VMEM((pairs, slices, 8, 2 * n), jnp.float32),
                pltpu.VMEM((pairs, slices, 8, 2 * n), jnp.float32),
                dma((CHUNKS,)), dma((CHUNKS,)),
                dma((CHUNKS,)), dma((CHUNKS,)),
                dma, dma,
                dma((REACH, CHUNKS)), dma((REACH, CHUNKS)),
                dma((pairs,)), dma((pairs,)),
            ],
            compiler_params=pltpu.CompilerParams(collective_id=0, has_side_effects=True),
        )(layers, jnp.transpose(offsets, (0, 2, 1)), subap_valid, defocus, weights, jnp.asarray(fr), jnp.asarray(fi), right)

    placed = (P("dir", "tile", None), P(), P("tile", None), P(), P())
    return jax.shard_map(
        shards, mesh=mesh, in_specs=placed, out_specs=P("dir", "tile", None, None), check_vma=False
    )
```
